32 devices in a mesh: seq: 8 (over z, y), head: 4 (over x, core).
Axes of the slice: x: 2, y: 2, z: 4, core: 2. Of those that a mesh axis runs over, the one named last changes fastest.
Arguments:
- query: bfloat16 [8, 40, 128], P(None, 'head'), may hold values from -400 to 400
- key_cache: bfloat16 [8, 4096, 8, 128], P(None, 'seq', 'head'), may hold values from -6 to 6
- value_cache: bfloat16 [8, 4096, 8, 128], P(None, 'seq', 'head'), may hold values from -6 to 6
- new_key: bfloat16 [8, 8, 128], P(None, 'head'), may hold values from -6 to 6
- new_value: bfloat16 [8, 8, 128], P(None, 'head'), may hold values from -6 to 6
- lengths: int32 [8], replicated, may hold values from 1024 to 4096, as said below
- out_weight: bfloat16 [5120, 5120], P('head', 'seq'), may hold values from -0.078125 to 0.078125
Outputs:
- projected: float32 [8, 5120], P(None, 'seq')
The draws below stay inside these ranges and needn't reach their ends.
Inputs may be any that keep to these rules, and one draw needn't show every extreme that they name: `lengths`: some sequence has exactly 4096 cached tokens.
All inputs are finite; a program needn't handle non-finite values.
Results may differ from the reference program's by a relative error of at most 0.0064.
Values sent between devices are 32-bit elements; how exact they have to be, the bound alone decides.
A program may use at most 64 MiB of HBM per device.

```python
import math
import jax
import jax.numpy as jnp
from jax import lax

B = 8
HQ = 40
KVH = 8
HD = 128
D = 5120
POS_DEV = 512
CACHE = 4096
STRETCH = 512
GROUP = 5
N_SEQ = 8


def common_noise(key):
    return jax.random.normal(jax.random.fold_in(key, 7), (B, HQ, HD), jnp.float32)


def draw_query(key, part):
    base = common_noise(key)
    return jnp.clip(3.0 * base, -18.0, 18.0).astype(jnp.bfloat16)


def draw_new_key(key, part):
    base = common_noise(key)
    grouped = base.reshape(B, KVH, HQ // KVH, HD).mean(axis=2)
    noise = jax.random.normal(jax.random.fold_in(key, 8), (B, KVH, HD), jnp.float32)
    return jnp.clip(1.8 * grouped + 0.6 * noise, -6.0, 6.0).astype(jnp.bfloat16)


def draw_lengths(key, part):
    drawn = jax.random.randint(jax.random.fold_in(key, 11), (B,), CACHE // 4, CACHE)
    picked = jax.random.randint(jax.random.fold_in(key, 12), (), 0, B)
    return jnp.where(jnp.arange(B) == picked, CACHE, drawn).astype(jnp.int32)


def levels(own_key, dims, split, low, largest):
    def one(position, blocks):
        draws = jax.random.uniform(jax.random.fold_in(jax.random.fold_in(own_key, 6), position), (blocks,), jnp.float32, low / len(split), largest / len(split))
        return jnp.repeat(jnp.exp(draws), dims[position] // blocks).reshape((-1,) + (1,) * (len(dims) - position - 1))

    gain = one(*split[0])
    for cut in split[1:]:
        gain = gain * one(*cut)
    return gain


def normal_values(own_key, dims, deviation, bound, split=(), held_as=jnp.bfloat16):
    entries = deviation * jax.random.normal(own_key, dims, jnp.float32)
    if split:
        entries = entries * levels(own_key, dims, split, -0.22, 0.18)
    return jnp.clip(entries, -bound, bound).astype(held_as)


def setup_inputs(seed: int = 0) -> dict:
    arg_keys = jax.random.split(jax.random.key(seed), 8)
    query = draw_query(jax.random.fold_in(arg_keys[7], 71), 0)
    key_cache = normal_values(arg_keys[1], (B, CACHE, KVH, HD), 1.0, 6.0, ((1, 8), (2, 4)))
    value_cache = normal_values(arg_keys[2], (B, CACHE, KVH, HD), 1.0, 6.0, ((1, 8), (2, 4)))
    new_key = draw_new_key(jax.random.fold_in(arg_keys[7], 71), 0)
    new_value = normal_values(arg_keys[4], (B, KVH, HD), 1.0, 6.0, ((1, 4),))
    lengths = draw_lengths(jax.random.fold_in(arg_keys[7], 71), 0)
    out_weight = normal_values(arg_keys[6], (HQ * HD, D), (HQ * HD) ** -0.5, 0.078125, ((0, 4), (1, 8)))
    return dict(query=query, key_cache=key_cache, value_cache=value_cache, new_key=new_key, new_value=new_value, lengths=lengths, out_weight=out_weight)


THETA_BASE = 10000000.0
NEG_FILL = -1e+30

def apply_rotary(values, positions):
    half_width = values.shape[-1] // 2
    frequency = jnp.exp(jnp.arange(half_width, dtype=jnp.float32) * jnp.float32(-2.0 * math.log(THETA_BASE) / values.shape[-1]))
    angles = positions[..., None] * frequency
    cos_part = jnp.cos(angles)
    sin_part = jnp.sin(angles)
    lower_section = values[..., :half_width]
    upper_half = values[..., half_width:]
    return jnp.concatenate([lower_section * cos_part - upper_half * sin_part, upper_half * cos_part + lower_section * sin_part], axis=-1)

def query_positions(lengths, stretch_len):
    remainder = lengths % stretch_len
    return jnp.stack([remainder, remainder + stretch_len, jnp.zeros_like(remainder) + (stretch_len + stretch_len // 2)], axis=-1).astype(jnp.float32)

def reference(query, key_cache, value_cache, new_key, new_value, lengths, out_weight):
    scaling = 1.0 / math.sqrt(HD)

    def one_sequence(per_seq):
        query_one, key_one, value_one, incoming_key, fresh_value, cache_length = per_seq
        query_pos = query_positions(cache_length, STRETCH)
        query_rot = apply_rotary(query_one.astype(jnp.float32)[None], query_pos[:, None]).astype(jnp.bfloat16)
        positions = jnp.arange(CACHE, dtype=jnp.int32)
        key_rot = apply_rotary(key_one.astype(jnp.float32), (positions % STRETCH).astype(jnp.float32)[:, None]).astype(jnp.bfloat16)
        query_by_group = query_rot.astype(jnp.float32).reshape(3, KVH, GROUP, HD)
        scores = jnp.einsum('vkgd,pkd->vkgp', query_by_group, key_rot.astype(jnp.float32)) * scaling
        query_stretch = cache_length // STRETCH
        key_stretch = positions // STRETCH
        key_class = jnp.where(key_stretch == query_stretch, 0, jnp.where(key_stretch == query_stretch - 1, 1, 2))
        selected_branch = jnp.where(key_class == 0, scores[0], jnp.where(key_class == 1, scores[1], scores[2]))
        live_mask = (positions < cache_length).reshape(N_SEQ, POS_DEV)
        blocks = jnp.where(live_mask, selected_branch.reshape(KVH, GROUP, N_SEQ, POS_DEV), NEG_FILL)
        block_max = lax.optimization_barrier(jnp.max(blocks, axis=-1))
        weights = jnp.where(live_mask, jnp.exp(blocks - block_max[..., None]), 0.0)
        block_total = lax.optimization_barrier(jnp.sum(weights, axis=-1))
        block_acc = jnp.einsum('kgnp,npkd->kgnd', weights.astype(jnp.bfloat16).astype(jnp.float32), value_one.astype(jnp.float32).reshape(N_SEQ, POS_DEV, KVH, HD))
        current_key = apply_rotary(incoming_key.astype(jnp.float32), query_pos[0]).astype(jnp.bfloat16)
        self_score = jnp.einsum('kgd,kd->kg', query_by_group[0], current_key.astype(jnp.float32)) * scaling
        top_score = jnp.maximum(self_score, lax.optimization_barrier(jnp.max(block_max, axis=-1)))
        factor = jnp.exp(block_max - top_score[..., None])
        self_factor = jnp.exp(self_score - top_score)
        total = self_factor + lax.optimization_barrier(jnp.sum(block_total * factor, axis=-1))
        accum = fresh_value.astype(jnp.float32)[:, None, :] * self_factor[..., None] + lax.optimization_barrier(jnp.sum(block_acc * factor[..., None], axis=2))
        return (accum / total[..., None]).reshape(HQ, HD).astype(jnp.bfloat16)
    attended = lax.map(one_sequence, (query, key_cache, value_cache, new_key, new_value, lengths))
    return jnp.dot(attended.reshape(B, HQ * HD), out_weight, preferred_element_type=jnp.float32)
```

```python
import functools
import math

import jax
import jax.numpy as jnp
from jax import lax
from jax.experimental import pallas as pl
from jax.experimental.pallas import tpu as pltpu
from jax.sharding import PartitionSpec as P

THETA_BASE = 10000000.0
NEG_FILL = -1e30
F32 = jnp.float32
BF16 = jnp.bfloat16
MESH = pl.DeviceIdType.MESH


def iota(shape, axis):
    return lax.broadcasted_iota(jnp.int32, shape, axis)


def rotate(x, cos, sin):
    return x * cos + pltpu.roll(x, x.shape[-1] // 2, x.ndim - 1) * sin


def kernel(
    seq_n, head_n, stretch,
    q_hbm, k_hbm, v_hbm, nk_hbm, nv_hbm, len_hbm, w_hbm,
    out_ref,
    q_in, kbuf, vbuf, nk_in, nv_in, lens, wbuf,
    cosv, sinv, cost, sint, q_pick, q_intra, nk_rot, nv_f32,
    send1, recv1, send2, recv2, recv3,
    in_sem, k_sem, v_sem, s1_sem, r1_sem, s2_sem, r2_sem, s3_sem, r3_sem,
):
    me = lax.axis_index("seq")
    mh = lax.axis_index("head")
    batch, rows2, hd = k_hbm.shape
    heads = q_hbm.shape[0]
    kv = nk_hbm.shape[0] // batch
    span = rows2 // kv
    group = heads // kv
    pad = send1.shape[1]
    half = hd // 2
    per_owner = seq_n // batch
    scaling = 1.0 / math.sqrt(hd)
    stat_row = heads
    stat_off = pad

    upper = me // (seq_n // 2)

    def far_first(k, n):
        return upper * k + (1 - upper) * (n - 1 - k)

    def copy_in(src, dst, sem):
        c = pltpu.make_async_copy(src, dst, sem)
        c.start()
        return c

    small = [
        copy_in(len_hbm, lens, in_sem.at[0]),
        copy_in(q_hbm, q_in, in_sem.at[1]),
        copy_in(nk_hbm, nk_in, in_sem.at[2]),
        copy_in(nv_hbm, nv_in, in_sem.at[3]),
    ]

    def k_copy(k):
        b = far_first(k, batch)
        return pltpu.make_async_copy(k_hbm.at[b], kbuf.at[k], k_sem.at[k])

    def v_copy(k):
        b = far_first(k, batch)
        return pltpu.make_async_copy(v_hbm.at[b], vbuf.at[k], v_sem.at[k])

    for k in range(batch):
        k_copy(k).start()
        v_copy(k).start()
    w_copy = copy_in(w_hbm, wbuf, in_sem.at[4])

    barrier = pltpu.get_barrier_semaphore()

    def greet(d, c):
        pl.semaphore_signal(
            barrier, inc=1, device_id=(lax.rem(me + d, seq_n), mh), device_id_type=MESH
        )
        return c

    lax.fori_loop(1, seq_n, greet, 0)
    for d in range(1, head_n):
        pl.semaphore_signal(
            barrier, inc=1, device_id=(me, lax.rem(mh + d, head_n)), device_id_type=MESH
        )

    def freq(shape):
        lane = iota(shape, len(shape) - 1)
        f = jnp.exp(
            (lane % half).astype(F32) * F32(-2.0 * math.log(THETA_BASE) / hd)
        )
        return f, jnp.where(lane < half, F32(-1.0), F32(1.0))

    tile = 8
    per_tile = tile // kv
    tiles = rows2 // tile
    start = lax.rem(me * span, stretch)
    f, sign = freq((tiles, hd))
    a = (start + iota((tiles, hd), 0) * per_tile).astype(F32) * f
    cosv[...] = jnp.cos(a)
    sinv[...] = jnp.sin(a) * sign
    f8, sign8 = freq((tile, hd))
    a8 = (iota((tile, hd), 0) // kv).astype(F32) * f8
    c0 = jnp.cos(a8)
    s0 = jnp.sin(a8) * sign8

    def fill(t, c):
        cv = cosv[pl.ds(t, 1), :]
        sv = sinv[pl.ds(t, 1), :]
        at = pl.ds(pl.multiple_of(t * tile, tile), tile)
        cost[at, :] = cv * c0 - sv * s0
        sint[at, :] = sv * c0 + cv * s0
        return c

    lax.fori_loop(0, tiles, fill, 0, unroll=8)

    for c in small:
        c.wait()
    row_b = iota((batch, hd), 0)
    lv = jnp.zeros((batch, hd), jnp.int32)
    for b in range(batch):
        lv = jnp.where(row_b == b, lens[b], lv)
    block_stretch = (me * span) // stretch
    rem = lax.rem(lv, stretch)
    qc = lax.div(lv, stretch)
    t_pick = jnp.where(
        qc == block_stretch,
        rem,
        jnp.where(qc - 1 == block_stretch, rem + stretch, stretch + stretch // 2),
    )
    fb, signb = freq((batch, hd))
    a_p = t_pick.astype(F32) * fb
    a_i = rem.astype(F32) * fb
    cp, sp = jnp.cos(a_p), jnp.sin(a_p) * signb
    ci, si = jnp.cos(a_i), jnp.sin(a_i) * signb
    for h in range(heads):
        x = q_in[h].astype(F32)
        q_pick[:, h, :] = rotate(x, cp, sp).astype(BF16).astype(F32)
        q_intra[:, h, :] = rotate(x, ci, si).astype(BF16).astype(F32)
    for h in range(heads, pad):
        q_pick[:, h, :] = jnp.zeros((batch, hd), F32)
        q_intra[:, h, :] = jnp.zeros((batch, hd), F32)
    row_n = iota((kv * batch, hd), 0)
    ln = jnp.zeros((kv * batch, hd), jnp.int32)
    for b in range(batch):
        ln = jnp.where(row_n // kv == b, lens[b], ln)
    fn, signn = freq((kv * batch, hd))
    a_n = lax.rem(ln, stretch).astype(F32) * fn
    nk_rot[...] = (
        rotate(nk_in[...].astype(F32), jnp.cos(a_n), jnp.sin(a_n) * signn).astype(BF16).astype(F32)
    )
    nv_f32[...] = nv_in[...].astype(F32)

    col = iota((pad, rows2), 1)
    fits = (col % kv) == (iota((pad, rows2), 0) // group)
    pos = me * span + col // kv
    prow = iota((pad, hd), 0)
    plane = iota((pad, hd), 1)
    diag = prow == plane
    diag2 = prow + stat_off == plane

    def send1_copy(k):
        b = far_first(k, batch)
        return pltpu.make_async_remote_copy(
            src_ref=send1.at[k],
            dst_ref=recv1.at[me],
            send_sem=s1_sem.at[k],
            recv_sem=r1_sem.at[me],
            device_id=(b * per_owner, mh),
            device_id_type=MESH,
        )

    chunk = min(256, rows2)

    def local_block(k):
        b = far_first(k, batch)
        k_copy(k).wait()
        q = q_pick[b].astype(BF16)
        parts = []
        for j in range(rows2 // chunk):
            at = pl.ds(j * chunk, chunk)
            kr = rotate(kbuf[k, at, :].astype(F32), cost[at, :], sint[at, :]).astype(BF16)
            parts.append(
                lax.dot_general(q, kr, (((1,), (1,)), ((), ())), preferred_element_type=F32)
            )
        s = jnp.concatenate(parts, axis=1) * scaling
        live = jnp.logical_and(fits, pos < lens[b])
        s = jnp.where(live, s, NEG_FILL)
        bmax = jnp.max(s, axis=1, keepdims=True)
        w = jnp.where(live, jnp.exp(s - bmax), 0.0)
        btot = jnp.sum(w, axis=1, keepdims=True)
        v_copy(k).wait()
        acc = jnp.dot(w.astype(BF16), vbuf[k], preferred_element_type=F32)
        stats = jnp.where(diag, bmax, jnp.where(diag2, btot, 0.0))
        stats = jnp.where(prow < heads, stats, 0.0)
        stats = jnp.sum(stats, axis=0, keepdims=True)
        return jnp.where(prow < heads, acc, jnp.where(prow == stat_row, stats, 0.0))

    for k in range(batch):
        payload = local_block(k)
        if k == 0:
            pl.semaphore_wait(barrier, seq_n - 1 + head_n - 1)
        mine = far_first(k, batch) * per_owner == me

        @pl.when(jnp.logical_not(mine))
        def _():
            send1[k] = payload
            send1_copy(k).start()

        @pl.when(mine)
        def _():
            recv1[me] = payload

    def send2_copy(d, slot):
        return pltpu.make_async_remote_copy(
            src_ref=send2,
            dst_ref=recv2.at[slot],
            send_sem=s2_sem.at[d],
            recv_sem=r2_sem.at[slot],
            device_id=(d, mh),
            device_id_type=MESH,
        )

    def over_peers(body):
        def step(j, c):
            d = far_first(j, seq_n)

            @pl.when(d != me)
            def _():
                body(d)

            return c

        lax.fori_loop(0, seq_n, step, 0, unroll=seq_n <= 8)

    def recv1_wait(d):
        pltpu.make_async_remote_copy(
            src_ref=recv1.at[d],
            dst_ref=recv1.at[d],
            send_sem=s1_sem.at[0],
            recv_sem=r1_sem.at[d],
            device_id=(d, mh),
            device_id_type=MESH,
        ).wait_recv()

    def combine():
        b = me // per_owner
        sc = jnp.sum(
            q_intra[b]
            * jnp.where(
                prow < group, nk_rot[pl.ds(b * kv, 1), :], nk_rot[pl.ds(b * kv + 1, 1), :]
            ),
            axis=1,
            keepdims=True,
        ) * scaling
        self_row = jnp.sum(jnp.where(diag, sc, 0.0), axis=0, keepdims=True)
        fresh = jnp.where(
            prow < group, nv_f32[pl.ds(b * kv, 1), :], nv_f32[pl.ds(b * kv + 1, 1), :]
        )
        over_peers(recv1_wait)
        st = recv1[:, stat_row, :]
        top = jnp.maximum(jnp.max(st, axis=0, keepdims=True), self_row)
        fac = jnp.exp(st - top)
        fac_self = jnp.exp(self_row - top)
        tot = pltpu.roll(st, hd - stat_off, 1)
        total = jnp.sum(tot * fac, axis=0, keepdims=True) + fac_self

        def column(r):
            return jnp.sum(jnp.where(diag, r, 0.0), axis=1, keepdims=True)

        acc = fresh * column(fac_self)
        for n in range(seq_n):
            acc = acc + recv1[n] * column(fac[n : n + 1, :])
        att = jnp.where(prow < heads, acc / column(jnp.where(plane[:1] < heads, total, 1.0)), 0.0)
        return att.astype(BF16).astype(F32), b

    def owner():
        att, b = combine()
        send2[...] = att
        over_peers(lambda d: send2_copy(d, b).start())
        recv2[b] = att

    if per_owner == 1:
        owner()
    else:
        pl.when(lax.rem(me, per_owner) == 0)(owner)

    def recv2_wait(b):
        pltpu.make_async_remote_copy(
            src_ref=send2,
            dst_ref=recv2.at[b],
            send_sem=s2_sem.at[0],
            recv_sem=r2_sem.at[b],
            device_id=(b * per_owner, mh),
            device_id_type=MESH,
        ).wait_recv()

    w_copy.wait()
    for k in range(batch):
        b = far_first(k, batch)

        @pl.when(b * per_owner != me)
        def _():
            recv2_wait(b)

    att = jnp.concatenate([recv2[:, h, :] for h in range(heads)], axis=1).astype(BF16)
    partial = jnp.dot(att, wbuf[...], preferred_element_type=F32)
    recv3[mh] = partial

    def send3_copy(d):
        return pltpu.make_async_remote_copy(
            src_ref=recv3.at[mh],
            dst_ref=recv3.at[mh],
            send_sem=s3_sem.at[d],
            recv_sem=r3_sem.at[mh],
            device_id=(me, lax.rem(mh + d, head_n)),
            device_id_type=MESH,
        )

    for d in range(1, head_n):
        send3_copy(d).start()
    for d in range(1, head_n):
        src = lax.rem(mh + d, head_n)
        pltpu.make_async_remote_copy(
            src_ref=recv3.at[src],
            dst_ref=recv3.at[src],
            send_sem=s3_sem.at[d],
            recv_sem=r3_sem.at[src],
            device_id=(me, src),
            device_id_type=MESH,
        ).wait_recv()
    total = recv3[0]
    for h in range(1, head_n):
        total = total + recv3[h]
    out_ref[...] = total

    for k in range(batch):

        @pl.when(far_first(k, batch) * per_owner != me)
        def _():
            send1_copy(k).wait_send()

    def sends2():
        over_peers(lambda d: send2_copy(d, me // per_owner).wait_send())

    if per_owner == 1:
        sends2()
    else:
        pl.when(lax.rem(me, per_owner) == 0)(sends2)
    for d in range(1, head_n):
        send3_copy(d).wait_send()


def body(query, key_cache, value_cache, new_key, new_value, lengths, out_weight):
    seq_n = lax.axis_size("seq")
    head_n = lax.axis_size("head")
    batch, span, kv, hd = key_cache.shape
    heads = query.shape[1]
    cols = out_weight.shape[1]
    stretch = span * seq_n // 8
    pad = -(-(heads + 1) // 8) * 8
    rows2 = span * kv
    dma = pltpu.SemaphoreType.DMA
    hbm = pl.BlockSpec(memory_space=pltpu.HBM)
    return pl.pallas_call(
        functools.partial(kernel, seq_n, head_n, stretch),
        out_shape=jax.ShapeDtypeStruct((batch, cols), F32),
        in_specs=[hbm] * 7,
        out_specs=pl.BlockSpec(memory_space=pltpu.VMEM),
        scratch_shapes=[
            pltpu.VMEM((heads, batch, hd), BF16),
            pltpu.VMEM((batch, rows2, hd), BF16),
            pltpu.VMEM((batch, rows2, hd), BF16),
            pltpu.VMEM((batch * kv, hd), BF16),
            pltpu.VMEM((batch * kv, hd), BF16),
            pltpu.SMEM((batch,), jnp.int32),
            pltpu.VMEM(out_weight.shape, BF16),
            pltpu.VMEM((rows2 // 8, hd), F32),
            pltpu.VMEM((rows2 // 8, hd), F32),
            pltpu.VMEM((rows2, hd), F32),
            pltpu.VMEM((rows2, hd), F32),
            pltpu.VMEM((batch, pad, hd), F32),
            pltpu.VMEM((batch, pad, hd), F32),
            pltpu.VMEM((batch * kv, hd), F32),
            pltpu.VMEM((batch * kv, hd), F32),
            pltpu.VMEM((batch, pad, hd), F32),
            pltpu.VMEM((seq_n, pad, hd), F32),
            pltpu.VMEM((pad, hd), F32),
            pltpu.VMEM((batch, pad, hd), F32),
            pltpu.VMEM((head_n, batch, cols), F32),
            dma((5,)),
            dma((batch,)),
            dma((batch,)),
            dma((batch,)),
            dma((seq_n,)),
            dma((seq_n,)),
            dma((batch,)),
            dma((head_n,)),
            dma((head_n,)),
        ],
        compiler_params=pltpu.CompilerParams(collective_id=0, has_side_effects=True),
    )(
        jnp.transpose(query, (1, 0, 2)),
        key_cache.reshape(batch, rows2, hd),
        value_cache.reshape(batch, rows2, hd),
        new_key.reshape(batch * kv, hd),
        new_value.reshape(batch * kv, hd),
        lengths,
        out_weight,
    )


def solution(mesh):
    placed = (
        P(None, "head", None),
        P(None, "seq", "head", None),
        P(None, "seq", "head", None),
        P(None, "head", None),
        P(None, "head", None),
        P(),
        P("head", "seq"),
    )
    return jax.shard_map(
        body, mesh=mesh, in_specs=placed, out_specs=P(None, "seq"), check_vma=False
    )
```

```python
import functools
import math

import jax
import jax.numpy as jnp
from jax import lax
from jax.experimental import pallas as pl
from jax.experimental.pallas import tpu as pltpu
from jax.sharding import PartitionSpec as P

THETA_BASE = 10000000.0
NEG_FILL = -1e30
F32 = jnp.float32
BF16 = jnp.bfloat16
MESH = pl.DeviceIdType.MESH


def iota(shape, axis):
    return lax.broadcasted_iota(jnp.int32, shape, axis)


def rotate(x, cos, sin):
    return x * cos + pltpu.roll(x, x.shape[-1] // 2, x.ndim - 1) * sin


def kernel(
    seq_n, head_n, stretch,
    q_hbm, k_hbm, v_hbm, nk_hbm, nv_hbm, len_hbm, w_hbm,
    out_ref,
    q_in, kbuf, vbuf, nk_in, nv_in, lens, wbuf,
    cosv, sinv, cost, sint, q_pick, q_intra, nk_rot, nv_f32,
    send1, recv1, send2, recv2, recv3,
    in_sem, k_sem, v_sem, s1_sem, r1_sem, s2_sem, r2_sem, s3_sem, r3_sem,
):
    me = lax.axis_index("seq")
    mh = lax.axis_index("head")
    batch, rows2, hd = k_hbm.shape
    heads = q_hbm.shape[0]
    kv = nk_hbm.shape[0] // batch
    span = rows2 // kv
    group = heads // kv
    pad = q_pick.shape[1]
    half = hd // 2
    per_owner = seq_n // batch
    scaling = 1.0 / math.sqrt(hd)
    stat_row = heads
    stat_off = pad

    away = sorted(range(1, batch), key=lambda d: -min(d, batch - d)) + [0]

    def turn(k):
        return lax.rem(me // per_owner + away[k], batch)

    def copy_in(src, dst, sem):
        c = pltpu.make_async_copy(src, dst, sem)
        c.start()
        return c

    small = [
        copy_in(len_hbm, lens, in_sem.at[0]),
        copy_in(q_hbm, q_in, in_sem.at[1]),
        copy_in(nk_hbm, nk_in, in_sem.at[2]),
        copy_in(nv_hbm, nv_in, in_sem.at[3]),
    ]

    def k_copy(k):
        b = turn(k)
        return pltpu.make_async_copy(k_hbm.at[b], kbuf.at[k], k_sem.at[k])

    def v_copy(k):
        b = turn(k)
        return pltpu.make_async_copy(v_hbm.at[b], vbuf.at[k], v_sem.at[k])

    for k in range(batch):
        k_copy(k).start()
        v_copy(k).start()
    w_copy = copy_in(w_hbm, wbuf, in_sem.at[4])

    barrier = pltpu.get_barrier_semaphore()

    def greet(d, c):
        pl.semaphore_signal(
            barrier, inc=1, device_id=(lax.rem(me + d, seq_n), mh), device_id_type=MESH
        )
        return c

    lax.fori_loop(1, seq_n, greet, 0)
    for d in range(1, head_n):
        pl.semaphore_signal(
            barrier, inc=1, device_id=(me, lax.rem(mh + d, head_n)), device_id_type=MESH
        )

    def freq(shape):
        lane = iota(shape, len(shape) - 1)
        f = jnp.exp(
            (lane % half).astype(F32) * F32(-2.0 * math.log(THETA_BASE) / hd)
        )
        return f, jnp.where(lane < half, F32(-1.0), F32(1.0))

    tile = 8
    per_tile = tile // kv
    tiles = rows2 // tile
    start = lax.rem(me * span, stretch)
    f, sign = freq((tiles, hd))
    a = (start + iota((tiles, hd), 0) * per_tile).astype(F32) * f
    cosv[...] = jnp.cos(a)
    sinv[...] = jnp.sin(a) * sign
    f8, sign8 = freq((tile, hd))
    a8 = (iota((tile, hd), 0) // kv).astype(F32) * f8
    c0 = jnp.cos(a8)
    s0 = jnp.sin(a8) * sign8

    def fill(t, c):
        cv = cosv[pl.ds(t, 1), :]
        sv = sinv[pl.ds(t, 1), :]
        at = pl.ds(pl.multiple_of(t * tile, tile), tile)
        cost[at, :] = cv * c0 - sv * s0
        sint[at, :] = sv * c0 + cv * s0
        return c

    lax.fori_loop(0, tiles, fill, 0, unroll=8)

    for c in small:
        c.wait()
    row_b = iota((batch, hd), 0)
    lv = jnp.zeros((batch, hd), jnp.int32)
    for b in range(batch):
        lv = jnp.where(row_b == b, lens[b], lv)
    block_stretch = (me * span) // stretch
    rem = lax.rem(lv, stretch)
    qc = lax.div(lv, stretch)
    t_pick = jnp.where(
        qc == block_stretch,
        rem,
        jnp.where(qc - 1 == block_stretch, rem + stretch, stretch + stretch // 2),
    )
    fb, signb = freq((batch, hd))
    a_p = t_pick.astype(F32) * fb
    a_i = rem.astype(F32) * fb
    cp, sp = jnp.cos(a_p), jnp.sin(a_p) * signb
    ci, si = jnp.cos(a_i), jnp.sin(a_i) * signb
    for h in range(heads):
        x = q_in[h].astype(F32)
        q_pick[:, h, :] = rotate(x, cp, sp).astype(BF16).astype(F32)
        q_intra[:, h, :] = rotate(x, ci, si).astype(BF16).astype(F32)
    for h in range(heads, pad):
        q_pick[:, h, :] = jnp.zeros((batch, hd), F32)
        q_intra[:, h, :] = jnp.zeros((batch, hd), F32)
    row_n = iota((kv * batch, hd), 0)
    ln = jnp.zeros((kv * batch, hd), jnp.int32)
    for b in range(batch):
        ln = jnp.where(row_n // kv == b, lens[b], ln)
    fn, signn = freq((kv * batch, hd))
    a_n = lax.rem(ln, stretch).astype(F32) * fn
    nk_rot[...] = (
        rotate(nk_in[...].astype(F32), jnp.cos(a_n), jnp.sin(a_n) * signn).astype(BF16).astype(F32)
    )
    nv_f32[...] = nv_in[...].astype(F32)

    col = iota((pad, rows2), 1)
    fits = (col % kv) == (iota((pad, rows2), 0) // group)
    pos = me * span + col // kv
    prow = iota((pad, hd), 0)
    plane = iota((pad, hd), 1)
    diag = prow == plane
    diag2 = prow + stat_off == plane

    def send1_copy(k):
        b = turn(k)
        return pltpu.make_async_remote_copy(
            src_ref=send1.at[k],
            dst_ref=recv1.at[me],
            send_sem=s1_sem.at[k],
            recv_sem=r1_sem.at[me],
            device_id=(b * per_owner, mh),
            device_id_type=MESH,
        )

    chunk = min(256, rows2)

    def local_blocks(ks):
        scores = []
        for k in ks:
            k_copy(k).wait()
            q = q_pick[turn(k)].astype(BF16)
            parts = []
            for j in range(rows2 // chunk):
                at = pl.ds(j * chunk, chunk)
                kr = rotate(kbuf[k, at, :].astype(F32), cost[at, :], sint[at, :]).astype(BF16)
                parts.append(
                    lax.dot_general(q, kr, (((1,), (1,)), ((), ())), preferred_element_type=F32)
                )
            scores.append(jnp.concatenate(parts, axis=1) * scaling)
        for k, s in zip(ks, scores):
            live = jnp.logical_and(fits, pos < lens[turn(k)])
            s = jnp.where(live, s, NEG_FILL)
            bmax = jnp.max(s, axis=1, keepdims=True)
            w = jnp.where(live, jnp.exp(s - bmax), 0.0)
            btot = jnp.sum(w, axis=1, keepdims=True)
            v_copy(k).wait()
            acc = jnp.dot(w.astype(BF16), vbuf[k], preferred_element_type=F32)
            stats = jnp.where(diag, bmax, jnp.where(diag2, btot, 0.0))
            stats = jnp.where(prow < heads, stats, 0.0)
            stats = jnp.sum(stats, axis=0, keepdims=True)
            send1[k] = jnp.where(prow < heads, acc, stats)[: heads + 1]

    together = 2
    for k in range(0, batch, together):
        local_blocks(range(k, min(k + together, batch)))
    pl.semaphore_wait(barrier, seq_n - 1 + head_n - 1)
    for k in range(batch - 1):
        send1_copy(k).start()
    if per_owner == 1:
        recv1[me] = send1[batch - 1]
    else:
        leads = lax.rem(me, per_owner) == 0

        @pl.when(jnp.logical_not(leads))
        def _():
            send1_copy(batch - 1).start()

        @pl.when(leads)
        def _():
            recv1[me] = send1[batch - 1]

    def send2_copy(d, slot):
        return pltpu.make_async_remote_copy(
            src_ref=send2,
            dst_ref=recv2.at[slot],
            send_sem=s2_sem.at[d],
            recv_sem=r2_sem.at[slot],
            device_id=(d, mh),
            device_id_type=MESH,
        )

    reach = sorted(range(1, seq_n), key=lambda d: -min(d, seq_n - d))

    def over_peers(body):
        if seq_n <= 8:
            for d in reach:
                body(lax.rem(me + d, seq_n))
        else:

            def step(d, c):
                body(lax.rem(me + d, seq_n))
                return c

            lax.fori_loop(1, seq_n, step, 0)

    def recv1_wait(d):
        pltpu.make_async_remote_copy(
            src_ref=recv1.at[d],
            dst_ref=recv1.at[d],
            send_sem=s1_sem.at[0],
            recv_sem=r1_sem.at[d],
            device_id=(d, mh),
            device_id_type=MESH,
        ).wait_recv()

    def combine():
        b = me // per_owner
        sc = jnp.sum(
            q_intra[b]
            * jnp.where(
                prow < group, nk_rot[pl.ds(b * kv, 1), :], nk_rot[pl.ds(b * kv + 1, 1), :]
            ),
            axis=1,
            keepdims=True,
        ) * scaling
        self_row = jnp.sum(jnp.where(diag, sc, 0.0), axis=0, keepdims=True)
        fresh = jnp.where(
            prow < group, nv_f32[pl.ds(b * kv, 1), :], nv_f32[pl.ds(b * kv + 1, 1), :]
        )
        over_peers(recv1_wait)
        st = recv1[:, stat_row, :]
        top = jnp.maximum(jnp.max(st, axis=0, keepdims=True), self_row)
        fac = jnp.exp(st - top)
        fac_self = jnp.exp(self_row - top)
        tot = pltpu.roll(st, hd - stat_off, 1)
        total = jnp.sum(tot * fac, axis=0, keepdims=True) + fac_self

        def column(r):
            return jnp.sum(jnp.where(diag[:heads], r, 0.0), axis=1, keepdims=True)

        acc = fresh[:heads] * column(fac_self)
        for n in range(seq_n):
            acc = acc + recv1[n, :heads, :] * column(fac[n : n + 1, :])
        att = acc / column(total)
        return att.astype(BF16).astype(F32), b

    def owner():
        att, b = combine()
        send2[...] = att
        over_peers(lambda d: send2_copy(d, b).start())
        recv2[b] = att

    if per_owner == 1:
        owner()
    else:
        pl.when(leads)(owner)

    def recv2_wait(b):
        pltpu.make_async_remote_copy(
            src_ref=send2,
            dst_ref=recv2.at[b],
            send_sem=s2_sem.at[0],
            recv_sem=r2_sem.at[b],
            device_id=(b * per_owner, mh),
            device_id_type=MESH,
        ).wait_recv()

    w_copy.wait()
    for k in range(batch - 1):
        recv2_wait(turn(k))
    if per_owner > 1:

        @pl.when(jnp.logical_not(leads))
        def _():
            recv2_wait(turn(batch - 1))

    att = jnp.concatenate([recv2[:, h, :] for h in range(heads)], axis=1).astype(BF16)
    partial = jnp.dot(att, wbuf[...], preferred_element_type=F32)
    recv3[mh] = partial

    def send3_copy(d):
        return pltpu.make_async_remote_copy(
            src_ref=recv3.at[mh],
            dst_ref=recv3.at[mh],
            send_sem=s3_sem.at[d],
            recv_sem=r3_sem.at[mh],
            device_id=(me, lax.rem(mh + d, head_n)),
            device_id_type=MESH,
        )

    for d in range(1, head_n):
        send3_copy(d).start()
    for d in range(1, head_n):
        src = lax.rem(mh + d, head_n)
        pltpu.make_async_remote_copy(
            src_ref=recv3.at[src],
            dst_ref=recv3.at[src],
            send_sem=s3_sem.at[d],
            recv_sem=r3_sem.at[src],
            device_id=(me, src),
            device_id_type=MESH,
        ).wait_recv()
    out_ref[...] = recv3[...]

    for k in range(batch - 1):
        send1_copy(k).wait_send()
    if per_owner > 1:

        @pl.when(jnp.logical_not(leads))
        def _():
            send1_copy(batch - 1).wait_send()

    def sends2():
        over_peers(lambda d: send2_copy(d, me // per_owner).wait_send())

    if per_owner == 1:
        sends2()
    else:
        pl.when(leads)(sends2)
    for d in range(1, head_n):
        send3_copy(d).wait_send()


def body(query, key_cache, value_cache, new_key, new_value, lengths, out_weight):
    seq_n = lax.axis_size("seq")
    head_n = lax.axis_size("head")
    batch, span, kv, hd = key_cache.shape
    heads = query.shape[1]
    cols = out_weight.shape[1]
    stretch = span * seq_n // 8
    pad = -(-(heads + 1) // 8) * 8
    rows2 = span * kv
    dma = pltpu.SemaphoreType.DMA
    hbm = pl.BlockSpec(memory_space=pltpu.HBM)
    res = pl.pallas_call(
        functools.partial(kernel, seq_n, head_n, stretch),
        out_shape=pltpu.VMEM((head_n, batch, cols), F32),
        in_specs=[hbm] * 7,
        out_specs=pl.BlockSpec(memory_space=pltpu.VMEM),
        scratch_shapes=[
            pltpu.VMEM((heads, batch, hd), BF16),
            pltpu.VMEM((batch, rows2, hd), BF16),
            pltpu.VMEM((batch, rows2, hd), BF16),
            pltpu.VMEM((batch * kv, hd), BF16),
            pltpu.VMEM((batch * kv, hd), BF16),
            pltpu.SMEM((batch,), jnp.int32),
            pltpu.VMEM(out_weight.shape, BF16),
            pltpu.VMEM((rows2 // 8, hd), F32),
            pltpu.VMEM((rows2 // 8, hd), F32),
            pltpu.VMEM((rows2, hd), F32),
            pltpu.VMEM((rows2, hd), F32),
            pltpu.VMEM((batch, pad, hd), F32),
            pltpu.VMEM((batch, pad, hd), F32),
            pltpu.VMEM((batch * kv, hd), F32),
            pltpu.VMEM((batch * kv, hd), F32),
            pltpu.VMEM((batch, heads + 1, hd), F32),
            pltpu.VMEM((seq_n, heads + 1, hd), F32),
            pltpu.VMEM((heads, hd), F32),
            pltpu.VMEM((batch, heads, hd), F32),
            pltpu.VMEM((head_n, batch, cols), F32),
            dma((5,)),
            dma((batch,)),
            dma((batch,)),
            dma((batch,)),
            dma((seq_n,)),
            dma((seq_n,)),
            dma((batch,)),
            dma((head_n,)),
            dma((head_n,)),
        ],
        compiler_params=pltpu.CompilerParams(collective_id=0, has_side_effects=True),
    )(
        jnp.transpose(query, (1, 0, 2)),
        key_cache.reshape(batch, rows2, hd),
        value_cache.reshape(batch, rows2, hd),
        new_key.reshape(batch * kv, hd),
        new_value.reshape(batch * kv, hd),
        lengths,
        out_weight,
    )
    return jnp.sum(res, axis=0)


def solution(mesh):
    placed = (
        P(None, "head", None),
        P(None, "seq", "head", None),
        P(None, "seq", "head", None),
        P(None, "head", None),
        P(None, "head", None),
        P(),
        P("head", "seq"),
    )
    return jax.shard_map(
        body, mesh=mesh, in_specs=placed, out_specs=P(None, "seq"), check_vma=False
    )
```

```python
import functools
import math

import jax
import jax.numpy as jnp
from jax import lax
from jax.experimental import pallas as pl
from jax.experimental.pallas import tpu as pltpu
from jax.sharding import PartitionSpec as P

THETA_BASE = 10000000.0
NEG_FILL = -1e30
F32 = jnp.float32
BF16 = jnp.bfloat16
MESH = pl.DeviceIdType.MESH


def iota(shape, axis):
    return lax.broadcasted_iota(jnp.int32, shape, axis)


def rotate(x, cos, sin):
    return x * cos + pltpu.roll(x, x.shape[-1] // 2, x.ndim - 1) * sin


def kernel(
    seq_n, head_n, stretch,
    q_hbm, k_hbm, v_hbm, nk_hbm, nv_hbm, len_hbm, w_hbm,
    out_ref,
    q_in, kbuf, vbuf, nk_in, nv_in, lens, wbuf,
    cosv, sinv, cost, sint, q_pick, q_intra, nk_rot, nv_f32,
    send1, recv1, send2, recv2, recv3,
    in_sem, k_sem, v_sem, s1_sem, r1_sem, s2_sem, r2_sem, s3_sem, r3_sem,
):
    me = lax.axis_index("seq")
    mh = lax.axis_index("head")
    batch, rows2, hd = k_hbm.shape
    heads = q_hbm.shape[0]
    kv = nk_hbm.shape[0] // batch
    span = rows2 // kv
    group = heads // kv
    pad = q_pick.shape[1]
    half = hd // 2
    per_owner = seq_n // batch
    scaling = 1.0 / math.sqrt(hd)
    stat_row = heads
    stat_off = pad

    away = sorted(range(1, batch), key=lambda d: -min(d, batch - d)) + [0]

    def turn(k):
        return lax.rem(me // per_owner + away[k], batch)

    def copy_in(src, dst, sem):
        c = pltpu.make_async_copy(src, dst, sem)
        c.start()
        return c

    small = [
        copy_in(len_hbm, lens, in_sem.at[0]),
        copy_in(q_hbm, q_in, in_sem.at[1]),
        copy_in(nk_hbm, nk_in, in_sem.at[2]),
        copy_in(nv_hbm, nv_in, in_sem.at[3]),
    ]

    def k_copy(k):
        b = turn(k)
        return pltpu.make_async_copy(k_hbm.at[b], kbuf.at[k], k_sem.at[k])

    def v_copy(k):
        b = turn(k)
        return pltpu.make_async_copy(v_hbm.at[b], vbuf.at[k], v_sem.at[k])

    for k in range(batch):
        k_copy(k).start()
        v_copy(k).start()
    w_copy = copy_in(w_hbm, wbuf, in_sem.at[4])

    barrier = pltpu.get_barrier_semaphore()

    def greet(d, c):
        pl.semaphore_signal(
            barrier, inc=1, device_id=(lax.rem(me + d, seq_n), mh), device_id_type=MESH
        )
        return c

    lax.fori_loop(1, seq_n, greet, 0)
    for d in range(1, head_n):
        pl.semaphore_signal(
            barrier, inc=1, device_id=(me, lax.rem(mh + d, head_n)), device_id_type=MESH
        )

    def freq(shape):
        lane = iota(shape, len(shape) - 1)
        f = jnp.exp(
            (lane % half).astype(F32) * F32(-2.0 * math.log(THETA_BASE) / hd)
        )
        return f, jnp.where(lane < half, F32(-1.0), F32(1.0))

    tile = 8
    per_tile = tile // kv
    tiles = rows2 // tile
    start = lax.rem(me * span, stretch)
    fine = min(16, tiles)
    coarse = tiles // fine
    ff, signf = freq((fine, hd))
    af = (iota((fine, hd), 0) * per_tile).astype(F32) * ff
    cf, sf = jnp.cos(af), jnp.sin(af)
    fc, _ = freq((coarse, hd))
    ac = (start + iota((coarse, hd), 0) * (fine * per_tile)).astype(F32) * fc
    cc, sc = jnp.cos(ac), jnp.sin(ac)
    for j in range(coarse):
        cr, sr = cc[j : j + 1], sc[j : j + 1]
        cosv[j * fine : (j + 1) * fine] = cr * cf - sr * sf
        sinv[j * fine : (j + 1) * fine] = (sr * cf + cr * sf) * signf
    f8, sign8 = freq((tile, hd))
    a8 = (iota((tile, hd), 0) // kv).astype(F32) * f8
    c0 = jnp.cos(a8)
    s0 = jnp.sin(a8) * sign8

    def fill(t, c):
        cv = cosv[pl.ds(t, 1), :]
        sv = sinv[pl.ds(t, 1), :]
        at = pl.ds(pl.multiple_of(t * tile, tile), tile)
        cost[at, :] = cv * c0 - sv * s0
        sint[at, :] = sv * c0 + cv * s0
        return c

    lax.fori_loop(0, tiles, fill, 0, unroll=8)

    for c in small:
        c.wait()
    row_b = iota((batch, hd), 0)
    lv = jnp.zeros((batch, hd), jnp.int32)
    for b in range(batch):
        lv = jnp.where(row_b == b, lens[b], lv)
    block_stretch = (me * span) // stretch
    rem = lax.rem(lv, stretch)
    qc = lax.div(lv, stretch)
    t_pick = jnp.where(
        qc == block_stretch,
        rem,
        jnp.where(qc - 1 == block_stretch, rem + stretch, stretch + stretch // 2),
    )
    fb, signb = freq((batch, hd))
    a_p = t_pick.astype(F32) * fb
    a_i = rem.astype(F32) * fb
    cp, sp = jnp.cos(a_p), jnp.sin(a_p) * signb
    ci, si = jnp.cos(a_i), jnp.sin(a_i) * signb
    for h in range(heads):
        x = q_in[h].astype(F32)
        q_pick[:, h, :] = rotate(x, cp, sp).astype(BF16).astype(F32)
        q_intra[:, h, :] = rotate(x, ci, si).astype(BF16).astype(F32)
    for h in range(heads, pad):
        q_pick[:, h, :] = jnp.zeros((batch, hd), F32)
        q_intra[:, h, :] = jnp.zeros((batch, hd), F32)
    row_n = iota((kv * batch, hd), 0)
    ln = jnp.zeros((kv * batch, hd), jnp.int32)
    for b in range(batch):
        ln = jnp.where(row_n // kv == b, lens[b], ln)
    fn, signn = freq((kv * batch, hd))
    a_n = lax.rem(ln, stretch).astype(F32) * fn
    nk_rot[...] = (
        rotate(nk_in[...].astype(F32), jnp.cos(a_n), jnp.sin(a_n) * signn).astype(BF16).astype(F32)
    )
    nv_f32[...] = nv_in[...].astype(F32)

    col = iota((pad, rows2), 1)
    fits = (col % kv) == (iota((pad, rows2), 0) // group)
    pos = me * span + col // kv
    prow = iota((pad, hd), 0)
    plane = iota((pad, hd), 1)
    diag = prow == plane
    diag2 = prow + stat_off == plane

    def send1_copy(k):
        b = turn(k)
        return pltpu.make_async_remote_copy(
            src_ref=send1.at[k],
            dst_ref=recv1.at[me],
            send_sem=s1_sem.at[k],
            recv_sem=r1_sem.at[me],
            device_id=(b * per_owner, mh),
            device_id_type=MESH,
        )

    chunk = min(256, rows2)

    def local_blocks(ks):
        scores = []
        for k in ks:
            k_copy(k).wait()
            q = q_pick[turn(k)].astype(BF16)
            parts = []
            for j in range(rows2 // chunk):
                at = pl.ds(j * chunk, chunk)
                kr = rotate(kbuf[k, at, :].astype(F32), cost[at, :], sint[at, :]).astype(BF16)
                parts.append(
                    lax.dot_general(q, kr, (((1,), (1,)), ((), ())), preferred_element_type=F32)
                )
            scores.append(jnp.concatenate(parts, axis=1) * scaling)
        for k, s in zip(ks, scores):
            live = jnp.logical_and(fits, pos < lens[turn(k)])
            s = jnp.where(live, s, NEG_FILL)
            bmax = jnp.max(s, axis=1, keepdims=True)
            w = jnp.where(live, jnp.exp(s - bmax), 0.0)
            btot = jnp.sum(w, axis=1, keepdims=True)
            v_copy(k).wait()
            acc = jnp.dot(w.astype(BF16), vbuf[k], preferred_element_type=F32)
            stats = jnp.where(diag, bmax, jnp.where(diag2, btot, 0.0))
            stats = jnp.where(prow < heads, stats, 0.0)
            stats = jnp.sum(stats, axis=0, keepdims=True)
            send1[k] = jnp.where(prow < heads, acc, stats)[: heads + 1]

    together = 2
    early = batch - together
    for k in range(0, batch, together):
        local_blocks(range(k, min(k + together, batch)))
        if k + together == early:
            pl.semaphore_wait(barrier, seq_n - 1 + head_n - 1)
            for j in range(early):
                send1_copy(j).start()
    for k in range(early, batch - 1):
        send1_copy(k).start()
    if per_owner == 1:
        recv1[me] = send1[batch - 1]
    else:
        leads = lax.rem(me, per_owner) == 0

        @pl.when(jnp.logical_not(leads))
        def _():
            send1_copy(batch - 1).start()

        @pl.when(leads)
        def _():
            recv1[me] = send1[batch - 1]

    def send2_copy(d, slot):
        return pltpu.make_async_remote_copy(
            src_ref=send2,
            dst_ref=recv2.at[slot],
            send_sem=s2_sem.at[d],
            recv_sem=r2_sem.at[slot],
            device_id=(d, mh),
            device_id_type=MESH,
        )

    reach = sorted(range(1, seq_n), key=lambda d: -min(d, seq_n - d))

    def over_peers(body):
        if seq_n <= 8:
            for d in reach:
                body(lax.rem(me + d, seq_n))
        else:

            def step(d, c):
                body(lax.rem(me + d, seq_n))
                return c

            lax.fori_loop(1, seq_n, step, 0)

    def recv1_wait(d):
        pltpu.make_async_remote_copy(
            src_ref=recv1.at[d],
            dst_ref=recv1.at[d],
            send_sem=s1_sem.at[0],
            recv_sem=r1_sem.at[d],
            device_id=(d, mh),
            device_id_type=MESH,
        ).wait_recv()

    def combine():
        b = me // per_owner
        sc = jnp.sum(
            q_intra[b]
            * jnp.where(
                prow < group, nk_rot[pl.ds(b * kv, 1), :], nk_rot[pl.ds(b * kv + 1, 1), :]
            ),
            axis=1,
            keepdims=True,
        ) * scaling
        self_row = jnp.sum(jnp.where(diag, sc, 0.0), axis=0, keepdims=True)
        fresh = jnp.where(
            prow < group, nv_f32[pl.ds(b * kv, 1), :], nv_f32[pl.ds(b * kv + 1, 1), :]
        )
        over_peers(recv1_wait)
        st = recv1[:, stat_row, :]
        top = jnp.maximum(jnp.max(st, axis=0, keepdims=True), self_row)
        fac = jnp.exp(st - top)
        fac_self = jnp.exp(self_row - top)
        tot = pltpu.roll(st, hd - stat_off, 1)
        total = jnp.sum(tot * fac, axis=0, keepdims=True) + fac_self

        def column(r):
            return jnp.sum(jnp.where(diag[:heads], r, 0.0), axis=1, keepdims=True)

        acc = fresh[:heads] * column(fac_self)
        for n in range(seq_n):
            acc = acc + recv1[n, :heads, :] * column(fac[n : n + 1, :])
        att = acc / column(total)
        return att.astype(BF16).astype(F32), b

    def owner():
        att, b = combine()
        send2[...] = att
        over_peers(lambda d: send2_copy(d, b).start())
        recv2[b] = att

    if per_owner == 1:
        owner()
    else:
        pl.when(leads)(owner)

    def recv2_wait(b):
        pltpu.make_async_remote_copy(
            src_ref=send2,
            dst_ref=recv2.at[b],
            send_sem=s2_sem.at[0],
            recv_sem=r2_sem.at[b],
            device_id=(b * per_owner, mh),
            device_id_type=MESH,
        ).wait_recv()

    w_copy.wait()
    for k in range(batch - 1):
        recv2_wait(turn(k))
    if per_owner > 1:

        @pl.when(jnp.logical_not(leads))
        def _():
            recv2_wait(turn(batch - 1))

    att = jnp.concatenate([recv2[:, h, :] for h in range(heads)], axis=1).astype(BF16)
    partial = jnp.dot(att, wbuf[...], preferred_element_type=F32)
    recv3[mh] = partial

    def send3_copy(d):
        return pltpu.make_async_remote_copy(
            src_ref=recv3.at[mh],
            dst_ref=recv3.at[mh],
            send_sem=s3_sem.at[d],
            recv_sem=r3_sem.at[mh],
            device_id=(me, lax.rem(mh + d, head_n)),
            device_id_type=MESH,
        )

    for d in range(1, head_n):
        send3_copy(d).start()
    for d in range(1, head_n):
        src = lax.rem(mh + d, head_n)
        pltpu.make_async_remote_copy(
            src_ref=recv3.at[src],
            dst_ref=recv3.at[src],
            send_sem=s3_sem.at[d],
            recv_sem=r3_sem.at[src],
            device_id=(me, src),
            device_id_type=MESH,
        ).wait_recv()
    out_ref[...] = recv3[...]

    for k in range(batch - 1):
        send1_copy(k).wait_send()
    if per_owner > 1:

        @pl.when(jnp.logical_not(leads))
        def _():
            send1_copy(batch - 1).wait_send()

    def sends2():
        over_peers(lambda d: send2_copy(d, me // per_owner).wait_send())

    if per_owner == 1:
        sends2()
    else:
        pl.when(leads)(sends2)
    for d in range(1, head_n):
        send3_copy(d).wait_send()


def body(query, key_cache, value_cache, new_key, new_value, lengths, out_weight):
    seq_n = lax.axis_size("seq")
    head_n = lax.axis_size("head")
    batch, span, kv, hd = key_cache.shape
    heads = query.shape[1]
    cols = out_weight.shape[1]
    stretch = span * seq_n // 8
    pad = -(-(heads + 1) // 8) * 8
    rows2 = span * kv
    dma = pltpu.SemaphoreType.DMA
    hbm = pl.BlockSpec(memory_space=pltpu.HBM)
    res = pl.pallas_call(
        functools.partial(kernel, seq_n, head_n, stretch),
        out_shape=pltpu.VMEM((head_n, batch, cols), F32),
        in_specs=[hbm] * 7,
        out_specs=pl.BlockSpec(memory_space=pltpu.VMEM),
        scratch_shapes=[
            pltpu.VMEM((heads, batch, hd), BF16),
            pltpu.VMEM((batch, rows2, hd), BF16),
            pltpu.VMEM((batch, rows2, hd), BF16),
            pltpu.VMEM((batch * kv, hd), BF16),
            pltpu.VMEM((batch * kv, hd), BF16),
            pltpu.SMEM((batch,), jnp.int32),
            pltpu.VMEM(out_weight.shape, BF16),
            pltpu.VMEM((rows2 // 8, hd), F32),
            pltpu.VMEM((rows2 // 8, hd), F32),
            pltpu.VMEM((rows2, hd), F32),
            pltpu.VMEM((rows2, hd), F32),
            pltpu.VMEM((batch, pad, hd), F32),
            pltpu.VMEM((batch, pad, hd), F32),
            pltpu.VMEM((batch * kv, hd), F32),
            pltpu.VMEM((batch * kv, hd), F32),
            pltpu.VMEM((batch, heads + 1, hd), F32),
            pltpu.VMEM((seq_n, heads + 1, hd), F32),
            pltpu.VMEM((heads, hd), F32),
            pltpu.VMEM((batch, heads, hd), F32),
            pltpu.VMEM((head_n, batch, cols), F32),
            dma((5,)),
            dma((batch,)),
            dma((batch,)),
            dma((batch,)),
            dma((seq_n,)),
            dma((seq_n,)),
            dma((batch,)),
            dma((head_n,)),
            dma((head_n,)),
        ],
        compiler_params=pltpu.CompilerParams(collective_id=0, has_side_effects=True),
    )(
        jnp.transpose(query, (1, 0, 2)),
        key_cache.reshape(batch, rows2, hd),
        value_cache.reshape(batch, rows2, hd),
        new_key.reshape(batch * kv, hd),
        new_value.reshape(batch * kv, hd),
        lengths,
        out_weight,
    )
    return jnp.sum(res, axis=0)


def solution(mesh):
    placed = (
        P(None, "head", None),
        P(None, "seq", "head", None),
        P(None, "seq", "head", None),
        P(None, "head", None),
        P(None, "head", None),
        P(),
        P("head", "seq"),
    )
    return jax.shard_map(
        body, mesh=mesh, in_specs=placed, out_specs=P(None, "seq"), check_vma=False
    )
```

```python
import functools
import math

import jax
import jax.numpy as jnp
from jax import lax
from jax.experimental import pallas as pl
from jax.experimental.pallas import tpu as pltpu
from jax.sharding import PartitionSpec as P

THETA_BASE = 10000000.0
NEG_FILL = -1e30
F32 = jnp.float32
BF16 = jnp.bfloat16
MESH = pl.DeviceIdType.MESH


def iota(shape, axis):
    return lax.broadcasted_iota(jnp.int32, shape, axis)


def rotate(x, cos, sin):
    return x * cos + pltpu.roll(x, x.shape[-1] // 2, x.ndim - 1) * sin


def kernel(
    seq_n, head_n, stretch,
    q_hbm, k_hbm, v_hbm, nk_hbm, nv_hbm, len_hbm, w_hbm,
    out_ref,
    q_in, kbuf, vbuf, nk_in, nv_in, lens, wbuf,
    cosv, sinv, cost, sint, q_pick, q_intra, nk_rot, nv_f32,
    send1, recv1, send2, recv2, recv3,
    in_sem, k_sem, v_sem, s1_sem, r1_sem, s2_sem, r2_sem, s3_sem, r3_sem,
):
    me = lax.axis_index("seq")
    mh = lax.axis_index("head")
    batch, rows2, hd = k_hbm.shape
    heads = q_hbm.shape[0]
    kv = nk_hbm.shape[0] // batch
    span = rows2 // kv
    group = heads // kv
    pad = q_pick.shape[1]
    half = hd // 2
    per_owner = seq_n // batch
    scaling = 1.0 / math.sqrt(hd)
    stat_row = heads
    stat_off = pad

    away = sorted(range(1, batch), key=lambda d: -min(d, batch - d)) + [0]

    def turn(k):
        return lax.rem(me // per_owner + away[k], batch)

    def copy_in(src, dst, sem):
        c = pltpu.make_async_copy(src, dst, sem)
        c.start()
        return c

    small = [
        copy_in(len_hbm, lens, in_sem.at[0]),
        copy_in(q_hbm, q_in, in_sem.at[1]),
        copy_in(nk_hbm, nk_in, in_sem.at[2]),
        copy_in(nv_hbm, nv_in, in_sem.at[3]),
    ]

    def k_copy(k):
        b = turn(k)
        return pltpu.make_async_copy(k_hbm.at[b], kbuf.at[k], k_sem.at[k])

    def v_copy(k):
        b = turn(k)
        return pltpu.make_async_copy(v_hbm.at[b], vbuf.at[k], v_sem.at[k])

    for k in range(batch):
        k_copy(k).start()
        v_copy(k).start()
    w_copy = copy_in(w_hbm, wbuf, in_sem.at[4])

    barrier = pltpu.get_barrier_semaphore()

    def greet(d, c):
        pl.semaphore_signal(
            barrier, inc=1, device_id=(lax.rem(me + d, seq_n), mh), device_id_type=MESH
        )
        return c

    lax.fori_loop(1, seq_n, greet, 0)
    for d in range(1, head_n):
        pl.semaphore_signal(
            barrier, inc=1, device_id=(me, lax.rem(mh + d, head_n)), device_id_type=MESH
        )

    def freq(shape):
        lane = iota(shape, len(shape) - 1)
        f = jnp.exp(
            (lane % half).astype(F32) * F32(-2.0 * math.log(THETA_BASE) / hd)
        )
        return f, jnp.where(lane < half, F32(-1.0), F32(1.0))

    tile = 8
    per_tile = tile // kv
    tiles = rows2 // tile
    start = lax.rem(me * span, stretch)
    fine = min(16, tiles)
    coarse = tiles // fine
    ff, signf = freq((fine, hd))
    af = (iota((fine, hd), 0) * per_tile).astype(F32) * ff
    cf, sf = jnp.cos(af), jnp.sin(af)
    fc, _ = freq((coarse, hd))
    ac = (start + iota((coarse, hd), 0) * (fine * per_tile)).astype(F32) * fc
    cc, sc = jnp.cos(ac), jnp.sin(ac)
    for j in range(coarse):
        cr, sr = cc[j : j + 1], sc[j : j + 1]
        cosv[j * fine : (j + 1) * fine] = cr * cf - sr * sf
        sinv[j * fine : (j + 1) * fine] = (sr * cf + cr * sf) * signf
    f8, sign8 = freq((tile, hd))
    a8 = (iota((tile, hd), 0) // kv).astype(F32) * f8
    c0 = jnp.cos(a8)
    s0 = jnp.sin(a8) * sign8

    def fill(t, c):
        cv = cosv[pl.ds(t, 1), :]
        sv = sinv[pl.ds(t, 1), :]
        at = pl.ds(pl.multiple_of(t * tile, tile), tile)
        cost[at, :] = cv * c0 - sv * s0
        sint[at, :] = sv * c0 + cv * s0
        return c

    lax.fori_loop(0, tiles, fill, 0, unroll=8)

    for c in small:
        c.wait()
    row_b = iota((batch, hd), 0)
    lv = jnp.zeros((batch, hd), jnp.int32)
    for b in range(batch):
        lv = jnp.where(row_b == b, lens[b], lv)
    block_stretch = (me * span) // stretch
    rem = lax.rem(lv, stretch)
    qc = lax.div(lv, stretch)
    t_pick = jnp.where(
        qc == block_stretch,
        rem,
        jnp.where(qc - 1 == block_stretch, rem + stretch, stretch + stretch // 2),
    )
    fb, signb = freq((batch, hd))
    a_p = t_pick.astype(F32) * fb
    a_i = rem.astype(F32) * fb
    cp, sp = jnp.cos(a_p), jnp.sin(a_p) * signb
    ci, si = jnp.cos(a_i), jnp.sin(a_i) * signb
    for h in range(heads):
        x = q_in[h].astype(F32)
        q_pick[:, h, :] = rotate(x, cp, sp).astype(BF16).astype(F32)
        q_intra[:, h, :] = rotate(x, ci, si).astype(BF16).astype(F32)
    for h in range(heads, pad):
        q_pick[:, h, :] = jnp.zeros((batch, hd), F32)
        q_intra[:, h, :] = jnp.zeros((batch, hd), F32)
    row_n = iota((kv * batch, hd), 0)
    ln = jnp.zeros((kv * batch, hd), jnp.int32)
    for b in range(batch):
        ln = jnp.where(row_n // kv == b, lens[b], ln)
    fn, signn = freq((kv * batch, hd))
    a_n = lax.rem(ln, stretch).astype(F32) * fn
    nk_rot[...] = (
        rotate(nk_in[...].astype(F32), jnp.cos(a_n), jnp.sin(a_n) * signn).astype(BF16).astype(F32)
    )
    nv_f32[...] = nv_in[...].astype(F32)

    col = iota((pad, rows2), 1)
    fits = (col % kv) == (iota((pad, rows2), 0) // group)
    pos = me * span + col // kv
    prow = iota((pad, hd), 0)
    plane = iota((pad, hd), 1)
    diag = prow == plane
    diag2 = prow + stat_off == plane

    def send1_copy(k):
        b = turn(k)
        return pltpu.make_async_remote_copy(
            src_ref=send1.at[k],
            dst_ref=recv1.at[me],
            send_sem=s1_sem.at[k],
            recv_sem=r1_sem.at[me],
            device_id=(b * per_owner, mh),
            device_id_type=MESH,
        )

    chunk = min(256, rows2)

    def local_blocks(ks):
        scores = []
        for k in ks:
            k_copy(k).wait()
            q = q_pick[turn(k)].astype(BF16)
            parts = []
            for j in range(rows2 // chunk):
                at = pl.ds(j * chunk, chunk)
                raw = kbuf[k, at, :]
                turned = pltpu.roll(raw, hd // 2, 1).astype(F32)
                kr = (raw.astype(F32) * cost[at, :] + turned * sint[at, :]).astype(BF16)
                parts.append(
                    lax.dot_general(q, kr, (((1,), (1,)), ((), ())), preferred_element_type=F32)
                )
            scores.append(jnp.concatenate(parts, axis=1) * scaling)
        for k, s in zip(ks, scores):
            live = jnp.logical_and(fits, pos < lens[turn(k)])
            s = jnp.where(live, s, NEG_FILL)
            bmax = jnp.max(s, axis=1, keepdims=True)
            w = jnp.where(live, jnp.exp(s - bmax), 0.0)
            btot = jnp.sum(w, axis=1, keepdims=True)
            v_copy(k).wait()
            acc = jnp.dot(w.astype(BF16), vbuf[k], preferred_element_type=F32)
            stats = jnp.where(diag, bmax, jnp.where(diag2, btot, 0.0))
            stats = jnp.where(prow < heads, stats, 0.0)
            stats = jnp.sum(stats, axis=0, keepdims=True)
            send1[k] = jnp.where(prow < heads, acc, stats)[: heads + 1]

    together = 2
    early = batch - together
    for k in range(0, batch, together):
        local_blocks(range(k, min(k + together, batch)))
        if k + together == early:
            pl.semaphore_wait(barrier, seq_n - 1 + head_n - 1)
            for j in range(early):
                send1_copy(j).start()
    for k in range(early, batch - 1):
        send1_copy(k).start()
    if per_owner == 1:
        recv1[me] = send1[batch - 1]
    else:
        leads = lax.rem(me, per_owner) == 0

        @pl.when(jnp.logical_not(leads))
        def _():
            send1_copy(batch - 1).start()

        @pl.when(leads)
        def _():
            recv1[me] = send1[batch - 1]

    def send2_copy(d, slot):
        return pltpu.make_async_remote_copy(
            src_ref=send2,
            dst_ref=recv2.at[slot],
            send_sem=s2_sem.at[d],
            recv_sem=r2_sem.at[slot],
            device_id=(d, mh),
            device_id_type=MESH,
        )

    reach = sorted(range(1, seq_n), key=lambda d: -min(d, seq_n - d))

    def over_peers(body):
        if seq_n <= 8:
            for d in reach:
                body(lax.rem(me + d, seq_n))
        else:

            def step(d, c):
                body(lax.rem(me + d, seq_n))
                return c

            lax.fori_loop(1, seq_n, step, 0)

    def recv1_wait(d):
        pltpu.make_async_remote_copy(
            src_ref=recv1.at[d],
            dst_ref=recv1.at[d],
            send_sem=s1_sem.at[0],
            recv_sem=r1_sem.at[d],
            device_id=(d, mh),
            device_id_type=MESH,
        ).wait_recv()

    def combine():
        b = me // per_owner
        sc = jnp.sum(
            q_intra[b]
            * jnp.where(
                prow < group, nk_rot[pl.ds(b * kv, 1), :], nk_rot[pl.ds(b * kv + 1, 1), :]
            ),
            axis=1,
            keepdims=True,
        ) * scaling
        self_row = jnp.sum(jnp.where(diag, sc, 0.0), axis=0, keepdims=True)
        fresh = jnp.where(
            prow < group, nv_f32[pl.ds(b * kv, 1), :], nv_f32[pl.ds(b * kv + 1, 1), :]
        )
        over_peers(recv1_wait)
        st = recv1[:, stat_row, :]
        top = jnp.maximum(jnp.max(st, axis=0, keepdims=True), self_row)
        fac = jnp.exp(st - top)
        fac_self = jnp.exp(self_row - top)
        tot = pltpu.roll(st, hd - stat_off, 1)
        total = jnp.sum(tot * fac, axis=0, keepdims=True) + fac_self

        def column(r):
            return jnp.sum(jnp.where(diag[:heads], r, 0.0), axis=1, keepdims=True)

        acc = fresh[:heads] * column(fac_self)
        for n in range(seq_n):
            acc = acc + recv1[n, :heads, :] * column(fac[n : n + 1, :])
        att = acc / column(total)
        return att.astype(BF16).astype(F32), b

    def owner():
        att, b = combine()
        send2[...] = att
        over_peers(lambda d: send2_copy(d, b).start())
        recv2[b] = att

    if per_owner == 1:
        owner()
    else:
        pl.when(leads)(owner)

    def recv2_wait(b):
        pltpu.make_async_remote_copy(
            src_ref=send2,
            dst_ref=recv2.at[b],
            send_sem=s2_sem.at[0],
            recv_sem=r2_sem.at[b],
            device_id=(b * per_owner, mh),
            device_id_type=MESH,
        ).wait_recv()

    w_copy.wait()
    for k in range(batch - 1):
        recv2_wait(turn(k))
    if per_owner > 1:

        @pl.when(jnp.logical_not(leads))
        def _():
            recv2_wait(turn(batch - 1))

    att = jnp.concatenate([recv2[:, h, :] for h in range(heads)], axis=1).astype(BF16)
    partial = jnp.dot(att, wbuf[...], preferred_element_type=F32)
    recv3[mh] = partial

    def send3_copy(d):
        return pltpu.make_async_remote_copy(
            src_ref=recv3.at[mh],
            dst_ref=recv3.at[mh],
            send_sem=s3_sem.at[d],
            recv_sem=r3_sem.at[mh],
            device_id=(me, lax.rem(mh + d, head_n)),
            device_id_type=MESH,
        )

    for d in range(1, head_n):
        send3_copy(d).start()
    for d in range(1, head_n):
        src = lax.rem(mh + d, head_n)
        pltpu.make_async_remote_copy(
            src_ref=recv3.at[src],
            dst_ref=recv3.at[src],
            send_sem=s3_sem.at[d],
            recv_sem=r3_sem.at[src],
            device_id=(me, src),
            device_id_type=MESH,
        ).wait_recv()
    out_ref[...] = recv3[...]

    for k in range(batch - 1):
        send1_copy(k).wait_send()
    if per_owner > 1:

        @pl.when(jnp.logical_not(leads))
        def _():
            send1_copy(batch - 1).wait_send()

    def sends2():
        over_peers(lambda d: send2_copy(d, me // per_owner).wait_send())

    if per_owner == 1:
        sends2()
    else:
        pl.when(leads)(sends2)
    for d in range(1, head_n):
        send3_copy(d).wait_send()


def body(query, key_cache, value_cache, new_key, new_value, lengths, out_weight):
    seq_n = lax.axis_size("seq")
    head_n = lax.axis_size("head")
    batch, span, kv, hd = key_cache.shape
    heads = query.shape[1]
    cols = out_weight.shape[1]
    stretch = span * seq_n // 8
    pad = -(-(heads + 1) // 8) * 8
    rows2 = span * kv
    dma = pltpu.SemaphoreType.DMA
    hbm = pl.BlockSpec(memory_space=pltpu.HBM)
    res = pl.pallas_call(
        functools.partial(kernel, seq_n, head_n, stretch),
        out_shape=pltpu.VMEM((head_n, batch, cols), F32),
        in_specs=[hbm] * 7,
        out_specs=pl.BlockSpec(memory_space=pltpu.VMEM),
        scratch_shapes=[
            pltpu.VMEM((heads, batch, hd), BF16),
            pltpu.VMEM((batch, rows2, hd), BF16),
            pltpu.VMEM((batch, rows2, hd), BF16),
            pltpu.VMEM((batch * kv, hd), BF16),
            pltpu.VMEM((batch * kv, hd), BF16),
            pltpu.SMEM((batch,), jnp.int32),
            pltpu.VMEM(out_weight.shape, BF16),
            pltpu.VMEM((rows2 // 8, hd), F32),
            pltpu.VMEM((rows2 // 8, hd), F32),
            pltpu.VMEM((rows2, hd), F32),
            pltpu.VMEM((rows2, hd), F32),
            pltpu.VMEM((batch, pad, hd), F32),
            pltpu.VMEM((batch, pad, hd), F32),
            pltpu.VMEM((batch * kv, hd), F32),
            pltpu.VMEM((batch * kv, hd), F32),
            pltpu.VMEM((batch, heads + 1, hd), F32),
            pltpu.VMEM((seq_n, heads + 1, hd), F32),
            pltpu.VMEM((heads, hd), F32),
            pltpu.VMEM((batch, heads, hd), F32),
            pltpu.VMEM((head_n, batch, cols), F32),
            dma((5,)),
            dma((batch,)),
            dma((batch,)),
            dma((batch,)),
            dma((seq_n,)),
            dma((seq_n,)),
            dma((batch,)),
            dma((head_n,)),
            dma((head_n,)),
        ],
        compiler_params=pltpu.CompilerParams(collective_id=0, has_side_effects=True),
    )(
        jnp.transpose(query, (1, 0, 2)),
        key_cache.reshape(batch, rows2, hd),
        value_cache.reshape(batch, rows2, hd),
        new_key.reshape(batch * kv, hd),
        new_value.reshape(batch * kv, hd),
        lengths,
        out_weight,
    )
    return jnp.sum(res, axis=0)


def solution(mesh):
    placed = (
        P(None, "head", None),
        P(None, "seq", "head", None),
        P(None, "seq", "head", None),
        P(None, "head", None),
        P(None, "head", None),
        P(),
        P("head", "seq"),
    )
    return jax.shard_map(
        body, mesh=mesh, in_specs=placed, out_specs=P(None, "seq"), check_vma=False
    )
```
